32 devices in a mesh: section: 4 (over y, core), dp: 8 (over z, x).
Axes of the slice: x: 2, y: 2, z: 4, core: 2. Of those that a mesh axis runs over, the one named last changes fastest.
Arguments:
- section_inputs: bfloat16 [4, 2, 1024, 1024], P('section', None, 'dp'), may hold values from -6 to 6
- gain: float32 [4, 1024], P('section'), may hold values from 0.25 to 1.75
- w_gate: bfloat16 [4, 1024, 1536], P('section'), may hold values from -0.1875 to 0.1875
- w_up: bfloat16 [4, 1024, 1536], P('section'), may hold values from -0.1875 to 0.1875
- w_out: bfloat16 [4, 1024, 1536], P('section'), may hold values from -0.15625 to 0.15625
- out_grad: bfloat16 [2, 1024, 1024], P(None, 'dp'), may hold values from -6 to 6
Outputs:
- grad_w_gate: float32 [4, 1024, 1536], P('section', 'dp')
- grad_w_up: float32 [4, 1024, 1536], P('section', 'dp')
- grad_w_out: float32 [4, 1024, 1536], P('section', 'dp')
- grad_gain: float32 [4, 1024], P('section', 'dp')
- input_grads: bfloat16 [4, 2, 1024, 1024], P('section', None, 'dp')
The draws below stay inside these ranges and needn't reach their ends.
All inputs are finite; a program needn't handle non-finite values.
Results may differ from the reference program's by a relative error of at most 0.014.
Values may be sent and summed in bfloat16 or wider, within the bound.
A program may use at most 128 MiB of HBM per device.

```python
import jax
import jax.numpy as jnp
from jax import lax

D = 1024
HID = 1536
MICRO = 2
TOK_DEV = 128
TOKENS = 1024
SECTIONS = 4
N_SECTION = 4


def with_spikes(values, own_key, source, target, blocks, factor):
    def block_of(axis_at):
        return (jnp.arange(values.shape[axis_at]) // (values.shape[axis_at] // blocks)).reshape((-1,) + (1,) * (values.ndim - 1 - axis_at))

    one_side = jax.random.permutation(own_key, blocks)[block_of(target)]
    other_side = (block_of(target) + blocks // 2) % blocks
    return jnp.where((block_of(source) == one_side) | (block_of(source) == other_side), factor * values, values)


def block_levels(own_key, dims, pieces, low, largest):
    factor_of, own = 1.0, jax.random.fold_in(own_key, 6)
    for dim, parts in pieces:
        draws = jnp.exp(jax.random.uniform(jax.random.fold_in(own, dim), (parts,), jnp.float32, low / len(pieces), largest / len(pieces)))
        factor_of = factor_of * jnp.repeat(draws, dims[dim] // parts).reshape([-1 if axis == dim else 1 for axis in range(len(dims))])
    return factor_of


def gaussian(own_key, extent, width, limit, shards=(), kind=jnp.bfloat16):
    drawn = width * jax.random.normal(own_key, extent, jnp.float32)
    if shards:
        drawn = drawn * block_levels(own_key, extent, shards, -0.22, 0.18)
    return jnp.clip(drawn, -limit, limit).astype(kind)


def noise_with(rng, shape, scale, reach, split, heavy, dtype=jnp.bfloat16):
    result = scale * jax.random.normal(rng, shape, jnp.float32)
    if split:
        result = result * block_levels(rng, shape, split, -0.22, 0.18)
    return jnp.clip(with_spikes(result, jax.random.fold_in(rng, 3), *heavy), -reach, reach).astype(dtype)


def setup_inputs(seed: int = 0) -> dict:
    seeds = jax.random.split(jax.random.key(seed), 7)
    section_inputs = noise_with(seeds[0], (SECTIONS, MICRO, TOKENS, D), 1.0, 6.0, ((0, 4), (2, 8)), (2, 3, 8, 2.0))
    gain = jnp.clip(1.0 + 0.15 * jax.random.normal(seeds[1], (SECTIONS, D), jnp.float32), 0.25, 1.75)
    w_gate = gaussian(seeds[2], (SECTIONS, D, HID), D ** -0.5, 0.1875, ((0, 4),))
    w_up = gaussian(seeds[3], (SECTIONS, D, HID), D ** -0.5, 0.1875, ((0, 4),))
    w_out = gaussian(seeds[4], (SECTIONS, D, HID), HID ** -0.5, 0.15625, ((0, 4),))
    out_grad = noise_with(seeds[5], (MICRO, TOKENS, D), 1.0, 6.0, ((1, 8),), (1, 2, 8, 2.0))
    return {"section_inputs": section_inputs, "gain": gain, "w_gate": w_gate, "w_up": w_up, "w_out": w_out, "out_grad": out_grad}


C_GELU = 0.7978845608028654
EPSILON = 1e-06

def gelu_parts(pre_act):
    cubic = 0.044715 * pre_act * pre_act * pre_act
    tangent = jnp.tanh(C_GELU * (pre_act + cubic))
    gelu_value = 0.5 * pre_act * (1.0 + tangent)
    gelu_slope = 0.5 * (1.0 + tangent) + 0.5 * pre_act * (1.0 - tangent * tangent) * C_GELU * (1.0 + 3.0 * 0.044715 * pre_act * pre_act)
    return (gelu_value, gelu_slope)

def section_back(inputs_row, incoming, gain_row, w_gate_mat, w_up_mat, w_out_mat):
    inputs_float = inputs_row.astype(jnp.float32)
    inverse_rms = lax.rsqrt(lax.optimization_barrier(jnp.mean(inputs_float * inputs_float, axis=-1, keepdims=True)) + EPSILON)
    normed = (inputs_float * inverse_rms * gain_row).astype(jnp.bfloat16)
    gate_pre = jnp.dot(normed, w_gate_mat, preferred_element_type=jnp.float32)
    up_pre = jnp.dot(normed, w_up_mat, preferred_element_type=jnp.float32)
    gelu_value, gelu_slope = gelu_parts(gate_pre)
    hidden_act = (gelu_value * up_pre).astype(jnp.bfloat16)
    act_grad = jnp.dot(incoming, w_out_mat, preferred_element_type=jnp.float32)
    gate_grad = (act_grad * up_pre * gelu_slope).astype(jnp.bfloat16)
    up_grad = (act_grad * gelu_value).astype(jnp.bfloat16)
    transpose_dims = (((1,), (1,)), ((), ()))
    normed_grad = lax.dot_general(gate_grad, w_gate_mat, transpose_dims, preferred_element_type=jnp.float32)
    normed_grad = normed_grad + lax.dot_general(up_grad, w_up_mat, transpose_dims, preferred_element_type=jnp.float32)
    gain_term = lax.optimization_barrier(jnp.sum(normed_grad * inputs_float * inverse_rms, axis=0))
    scaled_grad = normed_grad * gain_row
    input_grad = inverse_rms * scaled_grad - inputs_float * inverse_rms ** 3 * lax.optimization_barrier(jnp.mean(scaled_grad * inputs_float, axis=-1, keepdims=True))
    passed = (incoming.astype(jnp.float32) + input_grad).astype(jnp.bfloat16)
    return (passed, hidden_act, gate_grad, up_grad, normed, gain_term)

def reference(section_inputs, gain, w_gate, w_up, w_out, out_grad):
    token_scale = 1.0 / (MICRO * TOK_DEV)
    contract = (((0,), (0,)), ((), ()))
    grads_gate = []
    grads_up = []
    grads_out = []
    grads_gain = []
    passed_all = []
    incoming_all = out_grad
    for section_level in reversed(range(N_SECTION)):
        gate_sum = jnp.zeros((D, HID), jnp.float32)
        up_sum = jnp.zeros((D, HID), jnp.float32)
        out_sum = jnp.zeros((D, HID), jnp.float32)
        gain_sum = jnp.zeros((D,), jnp.float32)
        passed_list = []
        for member in range(MICRO):
            incoming = incoming_all[member]
            passed, hidden_act, gate_grad, up_grad, normed, gain_term = section_back(section_inputs[section_level, member], incoming, gain[section_level], w_gate[section_level], w_up[section_level], w_out[section_level])
            gate_sum = gate_sum + lax.dot_general(normed, gate_grad, contract, preferred_element_type=jnp.float32)
            up_sum = up_sum + lax.dot_general(normed, up_grad, contract, preferred_element_type=jnp.float32)
            out_sum = out_sum + lax.dot_general(incoming, hidden_act, contract, preferred_element_type=jnp.float32)
            gain_sum = gain_sum + gain_term
            passed_list.append(passed)
        incoming_all = jnp.stack(passed_list)
        passed_all.append(incoming_all)
        grads_gate.append(gate_sum * token_scale)
        grads_up.append(up_sum * token_scale)
        grads_out.append(out_sum * token_scale)
        grads_gain.append(gain_sum * token_scale)
    return (jnp.stack(grads_gate[::-1]), jnp.stack(grads_up[::-1]), jnp.stack(grads_out[::-1]), jnp.stack(grads_gain[::-1]), jnp.stack(passed_all[::-1]))
```

```python
import jax
import jax.numpy as jnp
from jax import lax
from jax.sharding import PartitionSpec as P

C_GELU = 0.7978845608028654
EPSILON = 1e-06


def from_behind(value, axis, steps):
    count = lax.axis_size(axis)
    leading, last = (max(0, -steps), min(count, count - steps))
    return lax.ppermute(value, axis, [(source, source + steps) for source in range(leading, last)])


def gelu_parts(pre_act):
    cubic = 0.044715 * pre_act * pre_act * pre_act
    tangent = jnp.tanh(C_GELU * (pre_act + cubic))
    gelu_value = 0.5 * pre_act * (1.0 + tangent)
    gelu_slope = 0.5 * (1.0 + tangent) + 0.5 * pre_act * (1.0 - tangent * tangent) * C_GELU * (
        1.0 + 3.0 * 0.044715 * pre_act * pre_act
    )
    return (gelu_value, gelu_slope)


def section_back(inputs_row, incoming, gain_row, w_gate_mat, w_up_mat, w_out_mat):
    inputs_float = inputs_row.astype(jnp.float32)
    inverse_rms = lax.rsqrt(jnp.mean(inputs_float * inputs_float, axis=-1, keepdims=True) + EPSILON)
    normed = (inputs_float * inverse_rms * gain_row).astype(jnp.bfloat16)
    gate_pre = jnp.dot(normed, w_gate_mat, preferred_element_type=jnp.float32)
    up_pre = jnp.dot(normed, w_up_mat, preferred_element_type=jnp.float32)
    gelu_value, gelu_slope = gelu_parts(gate_pre)
    hidden_act = (gelu_value * up_pre).astype(jnp.bfloat16)
    act_grad = jnp.dot(incoming, w_out_mat, preferred_element_type=jnp.float32)
    gate_grad = (act_grad * up_pre * gelu_slope).astype(jnp.bfloat16)
    up_grad = (act_grad * gelu_value).astype(jnp.bfloat16)
    transpose_dims = (((1,), (1,)), ((), ()))
    normed_grad = lax.dot_general(
        gate_grad, w_gate_mat, transpose_dims, preferred_element_type=jnp.float32
    )
    normed_grad = normed_grad + lax.dot_general(
        up_grad, w_up_mat, transpose_dims, preferred_element_type=jnp.float32
    )
    gain_term = jnp.sum(normed_grad * inputs_float * inverse_rms, axis=0)
    scaled_grad = normed_grad * gain_row
    input_grad = inverse_rms * scaled_grad - inputs_float * inverse_rms**3 * jnp.mean(
        scaled_grad * inputs_float, axis=-1, keepdims=True
    )
    passed = (incoming.astype(jnp.float32) + input_grad).astype(jnp.bfloat16)
    return (passed, hidden_act, gate_grad, up_grad, normed, gain_term)


def local_scatter(section_inputs, gain, w_gate, w_up, w_out, out_grad):
    section_count = lax.axis_size("section")
    position = lax.axis_index("section")
    inputs_here = section_inputs[0]
    gain_row = gain[0]
    w_gate_mat = w_gate[0]
    w_up_mat = w_up[0]
    w_out_mat = w_out[0]
    micro_count, tok_rows, model_width = inputs_here.shape
    hidden_width = w_gate_mat.shape[1]
    token_scale = 1.0 / (micro_count * tok_rows)

    def backward(inputs_row, incoming):
        return section_back(inputs_row, incoming, gain_row, w_gate_mat, w_up_mat, w_out_mat)

    narrow_rows = jnp.zeros((micro_count, tok_rows, model_width), jnp.bfloat16)
    wide_rows = jnp.zeros((micro_count, tok_rows, hidden_width), jnp.bfloat16)
    store = (
        narrow_rows,
        wide_rows,
        wide_rows,
        wide_rows,
        narrow_rows,
        narrow_rows,
        jnp.zeros((model_width,), jnp.float32),
    )

    def run_all(operand):
        incoming_all, previous = operand
        results = [
            backward(inputs_here[member], incoming_all[member]) for member in range(micro_count)
        ]
        gain_sum = results[0][5]
        member = 1
        gain_sum = gain_sum + results[member][5]
        stacked = tuple((jnp.stack([result[index] for result in results]) for index in range(5)))
        return stacked + (incoming_all, gain_sum)

    incoming_all = out_grad
    for section_level in reversed(range(section_count)):
        store = lax.cond(
            position == section_level, run_all, lambda operand: operand[1], (incoming_all, store)
        )
        if section_level > 0:
            incoming_all = from_behind(store[0], "section", -1)
    hidden_flat = store[1].reshape(-1, hidden_width)
    gate_flat = store[2].reshape(-1, hidden_width)
    up_flat = store[3].reshape(-1, hidden_width)
    normed_flat = store[4].reshape(-1, model_width)
    incoming_flat = store[5].reshape(-1, model_width)
    contract = (((0,), (0,)), ((), ()))
    gate_part = lax.dot_general(
        normed_flat, gate_flat, contract, preferred_element_type=jnp.float32
    )
    up_part = lax.dot_general(normed_flat, up_flat, contract, preferred_element_type=jnp.float32)
    out_part = lax.dot_general(
        incoming_flat, hidden_flat, contract, preferred_element_type=jnp.float32
    )
    all_rows = lax.psum_scatter(
        jnp.concatenate([gate_part, up_part, out_part], axis=1) * token_scale,
        "dp",
        scatter_dimension=0,
        tiled=True,
    )
    gate_rows = all_rows[:, :hidden_width]
    up_rows = all_rows[:, hidden_width : 2 * hidden_width]
    out_rows = all_rows[:, 2 * hidden_width :]
    gain_rows = lax.psum_scatter(store[6] * token_scale, "dp", scatter_dimension=0, tiled=True)
    return (gate_rows[None], up_rows[None], out_rows[None], gain_rows[None], store[0][None])


def forward_parts(rows, gain_row, w_gate_mat, w_up_mat):
    rows_float = rows.astype(jnp.float32)
    inverse_rms = lax.rsqrt(jnp.mean(rows_float * rows_float, axis=-1, keepdims=True) + EPSILON)
    normed = (rows_float * inverse_rms * gain_row).astype(jnp.bfloat16)
    gate_pre = jnp.dot(normed, w_gate_mat, preferred_element_type=jnp.float32)
    up_pre = jnp.dot(normed, w_up_mat, preferred_element_type=jnp.float32)
    gelu_value, gelu_slope = gelu_parts(gate_pre)
    hidden_act = (gelu_value * up_pre).astype(jnp.bfloat16)
    gate_factor = (up_pre * gelu_slope).astype(jnp.bfloat16)
    up_factor = gelu_value.astype(jnp.bfloat16)
    return (inverse_rms, normed, hidden_act, gate_factor, up_factor)


def local_gather(section_inputs, gain, w_gate, w_up, w_out, out_grad):
    section_count = lax.axis_size("section")
    position = lax.axis_index("section")
    replica = lax.axis_index("dp")
    replicas = lax.axis_size("dp")
    gain_row = gain[0]
    w_gate_mat = w_gate[0]
    w_up_mat = w_up[0]
    w_out_mat = w_out[0]
    _, micro_count, tok_rows, model_width = section_inputs.shape
    rows_own = micro_count * tok_rows
    token_scale = 1.0 / rows_own
    row_count = model_width // replicas
    rows = section_inputs[0].reshape(rows_own, model_width)
    rows_all = lax.all_gather(rows, "dp", axis=0, tiled=True)
    inverse_rms, _, _, gate_factor, up_factor = forward_parts(rows, gain_row, w_gate_mat, w_up_mat)
    transpose_dims = (((1,), (1,)), ((), ()))

    def stage(operand):
        incoming, _ = operand
        act_grad = jnp.dot(incoming, w_out_mat, preferred_element_type=jnp.float32)
        gate_grad = (act_grad * gate_factor).astype(jnp.bfloat16)
        up_grad = (act_grad * up_factor).astype(jnp.bfloat16)
        normed_grad = lax.dot_general(
            gate_grad, w_gate_mat, transpose_dims, preferred_element_type=jnp.float32
        ) + lax.dot_general(up_grad, w_up_mat, transpose_dims, preferred_element_type=jnp.float32)
        rows_float = rows.astype(jnp.float32)
        gain_term = jnp.sum(normed_grad * rows_float * inverse_rms, axis=0)
        scaled_grad = normed_grad * gain_row
        input_grad = inverse_rms * scaled_grad - rows_float * inverse_rms**3 * jnp.mean(
            scaled_grad * rows_float, axis=-1, keepdims=True
        )
        passed = (incoming.astype(jnp.float32) + input_grad).astype(jnp.bfloat16)
        return (passed, incoming, gain_term)

    incoming = out_grad.reshape(rows_own, model_width)
    store = (
        jnp.zeros((rows_own, model_width), jnp.bfloat16),
        jnp.zeros((rows_own, model_width), jnp.bfloat16),
        jnp.zeros((model_width,), jnp.float32),
    )
    for level in reversed(range(section_count)):
        store = lax.cond(
            position == level, stage, lambda operand: operand[1], (incoming, store)
        )
        if level > 0:
            incoming = lax.ppermute(store[0], "section", [(level, level - 1)])
    passed, incoming, gain_term = store
    incoming_all = lax.all_gather(incoming, "dp", axis=0, tiled=True)
    gain_all = lax.all_gather(gain_term, "dp", axis=0)
    _, normed_all, hidden_all, gate_factor_all, up_factor_all = forward_parts(
        rows_all, gain_row, w_gate_mat, w_up_mat
    )
    act_all = jnp.dot(incoming_all, w_out_mat, preferred_element_type=jnp.float32)
    gate_all = (act_all * gate_factor_all).astype(jnp.bfloat16)
    up_all = (act_all * up_factor_all).astype(jnp.bfloat16)
    own = replica * row_count
    normed_own = lax.dynamic_slice_in_dim(normed_all, own, row_count, axis=1)
    incoming_own = lax.dynamic_slice_in_dim(incoming_all, own, row_count, axis=1)
    contract = (((0,), (0,)), ((), ()))

    def grad_rows(left, right):
        total = lax.dot_general(left, right, contract, preferred_element_type=jnp.float32)
        return (total * token_scale)[None]

    gain_rows = lax.dynamic_slice_in_dim(gain_all, own, row_count, axis=1).sum(axis=0)
    return (
        grad_rows(normed_own, gate_all),
        grad_rows(normed_own, up_all),
        grad_rows(incoming_own, hidden_all),
        (gain_rows * token_scale)[None],
        passed.reshape(section_inputs.shape),
    )


def local(section_inputs, gain, w_gate, w_up, w_out, out_grad):
    _, micro_count, tok_rows, _ = section_inputs.shape
    gathered_rows = lax.axis_size("dp") * micro_count * tok_rows
    plan = local_gather if 2 * gathered_rows <= 3 * w_gate.shape[2] else local_scatter
    return plan(section_inputs, gain, w_gate, w_up, w_out, out_grad)


def solution(mesh):
    placed = (
        P("section", None, "dp", None),
        P("section", None),
        P("section", None, None),
        P("section", None, None),
        P("section", None, None),
        P(None, "dp", None),
    )
    return jax.shard_map(
        local,
        mesh=mesh,
        in_specs=placed,
        out_specs=(
            P("section", "dp", None),
            P("section", "dp", None),
            P("section", "dp", None),
            P("section", "dp"),
            P("section", None, "dp", None),
        ),
        check_vma=False,
    )
```

```python
import jax
import jax.numpy as jnp
from jax import lax
from jax.experimental import pallas as pl
from jax.experimental.pallas import tpu as pltpu
from jax.sharding import PartitionSpec as P

C_GELU = 0.7978845608028654
EPSILON = 1e-06


def from_behind(value, axis, steps):
    count = lax.axis_size(axis)
    leading, last = (max(0, -steps), min(count, count - steps))
    return lax.ppermute(value, axis, [(source, source + steps) for source in range(leading, last)])


def gelu_parts(pre_act):
    cubic = 0.044715 * pre_act * pre_act * pre_act
    tangent = jnp.tanh(C_GELU * (pre_act + cubic))
    gelu_value = 0.5 * pre_act * (1.0 + tangent)
    gelu_slope = 0.5 * (1.0 + tangent) + 0.5 * pre_act * (1.0 - tangent * tangent) * C_GELU * (
        1.0 + 3.0 * 0.044715 * pre_act * pre_act
    )
    return (gelu_value, gelu_slope)


def section_back(inputs_row, incoming, gain_row, w_gate_mat, w_up_mat, w_out_mat):
    inputs_float = inputs_row.astype(jnp.float32)
    inverse_rms = lax.rsqrt(jnp.mean(inputs_float * inputs_float, axis=-1, keepdims=True) + EPSILON)
    normed = (inputs_float * inverse_rms * gain_row).astype(jnp.bfloat16)
    gate_pre = jnp.dot(normed, w_gate_mat, preferred_element_type=jnp.float32)
    up_pre = jnp.dot(normed, w_up_mat, preferred_element_type=jnp.float32)
    gelu_value, gelu_slope = gelu_parts(gate_pre)
    hidden_act = (gelu_value * up_pre).astype(jnp.bfloat16)
    act_grad = jnp.dot(incoming, w_out_mat, preferred_element_type=jnp.float32)
    gate_grad = (act_grad * up_pre * gelu_slope).astype(jnp.bfloat16)
    up_grad = (act_grad * gelu_value).astype(jnp.bfloat16)
    transpose_dims = (((1,), (1,)), ((), ()))
    normed_grad = lax.dot_general(
        gate_grad, w_gate_mat, transpose_dims, preferred_element_type=jnp.float32
    )
    normed_grad = normed_grad + lax.dot_general(
        up_grad, w_up_mat, transpose_dims, preferred_element_type=jnp.float32
    )
    gain_term = jnp.sum(normed_grad * inputs_float * inverse_rms, axis=0)
    scaled_grad = normed_grad * gain_row
    input_grad = inverse_rms * scaled_grad - inputs_float * inverse_rms**3 * jnp.mean(
        scaled_grad * inputs_float, axis=-1, keepdims=True
    )
    passed = (incoming.astype(jnp.float32) + input_grad).astype(jnp.bfloat16)
    return (passed, hidden_act, gate_grad, up_grad, normed, gain_term)


def local_scatter(section_inputs, gain, w_gate, w_up, w_out, out_grad):
    section_count = lax.axis_size("section")
    position = lax.axis_index("section")
    inputs_here = section_inputs[0]
    gain_row = gain[0]
    w_gate_mat = w_gate[0]
    w_up_mat = w_up[0]
    w_out_mat = w_out[0]
    micro_count, tok_rows, model_width = inputs_here.shape
    hidden_width = w_gate_mat.shape[1]
    token_scale = 1.0 / (micro_count * tok_rows)

    def backward(inputs_row, incoming):
        return section_back(inputs_row, incoming, gain_row, w_gate_mat, w_up_mat, w_out_mat)

    narrow_rows = jnp.zeros((micro_count, tok_rows, model_width), jnp.bfloat16)
    wide_rows = jnp.zeros((micro_count, tok_rows, hidden_width), jnp.bfloat16)
    store = (
        narrow_rows,
        wide_rows,
        wide_rows,
        wide_rows,
        narrow_rows,
        narrow_rows,
        jnp.zeros((model_width,), jnp.float32),
    )

    def run_all(operand):
        incoming_all, previous = operand
        results = [
            backward(inputs_here[member], incoming_all[member]) for member in range(micro_count)
        ]
        gain_sum = results[0][5]
        member = 1
        gain_sum = gain_sum + results[member][5]
        stacked = tuple((jnp.stack([result[index] for result in results]) for index in range(5)))
        return stacked + (incoming_all, gain_sum)

    incoming_all = out_grad
    for section_level in reversed(range(section_count)):
        store = lax.cond(
            position == section_level, run_all, lambda operand: operand[1], (incoming_all, store)
        )
        if section_level > 0:
            incoming_all = from_behind(store[0], "section", -1)
    hidden_flat = store[1].reshape(-1, hidden_width)
    gate_flat = store[2].reshape(-1, hidden_width)
    up_flat = store[3].reshape(-1, hidden_width)
    normed_flat = store[4].reshape(-1, model_width)
    incoming_flat = store[5].reshape(-1, model_width)
    contract = (((0,), (0,)), ((), ()))
    gate_part = lax.dot_general(
        normed_flat, gate_flat, contract, preferred_element_type=jnp.float32
    )
    up_part = lax.dot_general(normed_flat, up_flat, contract, preferred_element_type=jnp.float32)
    out_part = lax.dot_general(
        incoming_flat, hidden_flat, contract, preferred_element_type=jnp.float32
    )
    all_rows = lax.psum_scatter(
        jnp.concatenate([gate_part, up_part, out_part], axis=1) * token_scale,
        "dp",
        scatter_dimension=0,
        tiled=True,
    )
    gate_rows = all_rows[:, :hidden_width]
    up_rows = all_rows[:, hidden_width : 2 * hidden_width]
    out_rows = all_rows[:, 2 * hidden_width :]
    gain_rows = lax.psum_scatter(store[6] * token_scale, "dp", scatter_dimension=0, tiled=True)
    return (gate_rows[None], up_rows[None], out_rows[None], gain_rows[None], store[0][None])


def forward_parts(rows, gain_row, w_gate_mat, w_up_mat):
    rows_float = rows.astype(jnp.float32)
    inverse_rms = lax.rsqrt(jnp.mean(rows_float * rows_float, axis=-1, keepdims=True) + EPSILON)
    normed = (rows_float * inverse_rms * gain_row).astype(jnp.bfloat16)
    gate_pre = jnp.dot(normed, w_gate_mat, preferred_element_type=jnp.float32)
    up_pre = jnp.dot(normed, w_up_mat, preferred_element_type=jnp.float32)
    gelu_value, gelu_slope = gelu_parts(gate_pre)
    hidden_act = (gelu_value * up_pre).astype(jnp.bfloat16)
    gate_factor = (up_pre * gelu_slope).astype(jnp.bfloat16)
    up_factor = gelu_value.astype(jnp.bfloat16)
    return (inverse_rms, normed, hidden_act, gate_factor, up_factor)


def grad_kernel(token_scale, g_ref, normed_ref, hidden_ref, gate_ref, up_ref, wo_ref, *rest):
    sums = rest

    @pl.when(pl.program_id(0) == 0)
    def _():
        for target in sums:
            target[...] = jnp.zeros_like(target)

    row_count = sums[0].shape[0]
    hidden_width = wo_ref.shape[1]
    own = pl.ds(pl.multiple_of(lax.axis_index("dp") * row_count, row_count), row_count)
    incoming = g_ref[...]
    incoming_own = g_ref[:, own]
    normed_own = normed_ref[...]
    chunk = 512 if hidden_width % 512 == 0 else hidden_width

    def add_rows(target, columns, left, right):
        term = lax.dot_general(
            left, right, (((0,), (0,)), ((), ())), preferred_element_type=jnp.float32
        )
        target[:, columns] += term * token_scale

    for start in range(0, hidden_width, chunk):
        columns = slice(start, start + chunk)
        act_grad = jnp.dot(incoming, wo_ref[:, columns], preferred_element_type=jnp.float32)
        gate_grad = (act_grad * gate_ref[:, columns].astype(jnp.float32)).astype(jnp.bfloat16)
        up_grad = (act_grad * up_ref[:, columns].astype(jnp.float32)).astype(jnp.bfloat16)
        add_rows(sums[0], columns, normed_own, gate_grad)
        add_rows(sums[1], columns, normed_own, up_grad)
        add_rows(sums[2], columns, incoming_own, hidden_ref[:, columns])


def grad_rows_of(incoming, normed_own, hidden, gate_factor, up_factor, w_out_mat, token_scale):
    rows, model_width = incoming.shape
    hidden_width = w_out_mat.shape[1]
    row_count = normed_own.shape[1]
    block = 256 if rows % 256 == 0 else rows

    def tokens(width):
        return pl.BlockSpec((block, width), lambda i: (i, 0))

    def fixed(shape):
        return pl.BlockSpec(shape, lambda i: (0, 0))

    total = fixed((row_count, hidden_width))
    return pl.pallas_call(
        lambda *refs: grad_kernel(token_scale, *refs),
        name="grad_rows",
        grid=(rows // block,),
        in_specs=[tokens(model_width), tokens(row_count)]
        + [tokens(hidden_width)] * 3
        + [fixed((model_width, hidden_width))],
        out_specs=[total] * 3,
        out_shape=[jax.ShapeDtypeStruct((row_count, hidden_width), jnp.float32)] * 3,
        compiler_params=pltpu.CompilerParams(vmem_limit_bytes=40 * 1024 * 1024),
        cost_estimate=pl.CostEstimate(
            flops=2 * rows * (model_width + 3 * row_count) * hidden_width,
            bytes_accessed=6 * rows * hidden_width + 12 * row_count * hidden_width,
            transcendentals=0,
        ),
    )(incoming, normed_own, hidden, gate_factor, up_factor, w_out_mat)


def local_gather(section_inputs, gain, w_gate, w_up, w_out, out_grad):
    section_count = lax.axis_size("section")
    position = lax.axis_index("section")
    replica = lax.axis_index("dp")
    replicas = lax.axis_size("dp")
    gain_row = gain[0]
    w_gate_mat = w_gate[0]
    w_up_mat = w_up[0]
    w_out_mat = w_out[0]
    _, micro_count, tok_rows, model_width = section_inputs.shape
    rows_own = micro_count * tok_rows
    token_scale = 1.0 / rows_own
    row_count = model_width // replicas
    rows = section_inputs[0].reshape(rows_own, model_width)
    rows_all = lax.all_gather(rows, "dp", axis=0, tiled=True)
    inverse_rms, _, _, gate_factor, up_factor = forward_parts(rows, gain_row, w_gate_mat, w_up_mat)
    transpose_dims = (((1,), (1,)), ((), ()))

    def stage(operand):
        incoming, _ = operand
        act_grad = jnp.dot(incoming, w_out_mat, preferred_element_type=jnp.float32)
        gate_grad = (act_grad * gate_factor).astype(jnp.bfloat16)
        up_grad = (act_grad * up_factor).astype(jnp.bfloat16)
        normed_grad = lax.dot_general(
            gate_grad, w_gate_mat, transpose_dims, preferred_element_type=jnp.float32
        ) + lax.dot_general(up_grad, w_up_mat, transpose_dims, preferred_element_type=jnp.float32)
        rows_float = rows.astype(jnp.float32)
        gain_term = jnp.sum(normed_grad * rows_float * inverse_rms, axis=0)
        scaled_grad = normed_grad * gain_row
        input_grad = inverse_rms * scaled_grad - rows_float * inverse_rms**3 * jnp.mean(
            scaled_grad * rows_float, axis=-1, keepdims=True
        )
        passed = (incoming.astype(jnp.float32) + input_grad).astype(jnp.bfloat16)
        return (passed, gain_term)

    incoming = out_grad.reshape(rows_own, model_width)
    store = (
        jnp.zeros((rows_own, model_width), jnp.bfloat16),
        jnp.zeros((model_width,), jnp.float32),
    )
    for level in reversed(range(section_count)):
        store = lax.cond(position == level, stage, lambda operand: operand[1], (incoming, store))
        if level > 0:
            received = lax.ppermute(store[0], "section", [(level, level - 1)])
            incoming = jnp.where(position == level - 1, received, incoming)
    passed, gain_sum = store

    incoming_all = lax.all_gather(incoming, "dp", axis=0, tiled=True)
    own = replica * row_count
    _, normed, hidden, gate_all, up_all = forward_parts(rows_all, gain_row, w_gate_mat, w_up_mat)
    normed_own = lax.dynamic_slice_in_dim(normed, own, row_count, axis=1)
    sums = grad_rows_of(
        incoming_all, normed_own, hidden, gate_all, up_all, w_out_mat, token_scale
    )
    gain_all = lax.all_gather(gain_sum, "dp", axis=0)
    gain_rows = lax.dynamic_slice_in_dim(gain_all, own, row_count, axis=1).sum(axis=0)
    return (
        sums[0][None],
        sums[1][None],
        sums[2][None],
        (gain_rows * token_scale)[None],
        passed.reshape(section_inputs.shape),
    )


def local(section_inputs, gain, w_gate, w_up, w_out, out_grad):
    _, micro_count, tok_rows, _ = section_inputs.shape
    gathered_rows = lax.axis_size("dp") * micro_count * tok_rows
    small = lax.axis_size("dp") % 2 == 0 and 2 * gathered_rows <= 3 * w_gate.shape[2]
    plan = local_gather if small else local_scatter
    return plan(section_inputs, gain, w_gate, w_up, w_out, out_grad)


def solution(mesh):
    placed = (
        P("section", None, "dp", None),
        P("section", None),
        P("section", None, None),
        P("section", None, None),
        P("section", None, None),
        P(None, "dp", None),
    )
    return jax.shard_map(
        local,
        mesh=mesh,
        in_specs=placed,
        out_specs=(
            P("section", "dp", None),
            P("section", "dp", None),
            P("section", "dp", None),
            P("section", "dp"),
            P("section", None, "dp", None),
        ),
        check_vma=False,
    )
```
